32 devices in a mesh: px: 8 (over z, y), py: 4 (over x, core).
Axes of the slice: x: 2, y: 2, z: 4, core: 2. Of those that a mesh axis runs over, the one named last changes fastest.
Arguments:
- field: bfloat16 [1, 32, 128, 128, 256], P(None, None, 'px', 'py'), may hold values from -6 to 6
- spectral_weight: bfloat16 [2, 32, 32, 32, 64, 64], P(None, None, 'px', 'py'), may hold values from -72 to 72
- point_weight: bfloat16 [32, 32], replicated, may hold values from -1 to 1
- point_bias: float32 [32], replicated, may hold values from -3 to 3
Outputs:
- layer_out: bfloat16 [1, 32, 128, 128, 256], P(None, None, 'px', 'py')
The draws below stay inside these ranges and needn't reach their ends.
All inputs are finite; a program needn't handle non-finite values.
Results may differ from the reference program's by a relative error of at most 0.0085.
Values may be sent and summed in bfloat16 or wider, within the bound.
A program may use at most 192 MiB of HBM per device.

```python
import jax
import jax.numpy as jnp
from jax import lax

C = 32
MX = 64
MY = 64
MZ = 32
NZ = 256
B = 1
NX = 128
NY = 128


def draw_spectral_weight(key, part):
    normal_draw = jnp.clip(jax.random.normal(key, (2, C, C, MZ, MX, MY), jnp.float32), -6.0, 6.0)
    values = 2.0 * normal_draw
    return values.astype(jnp.bfloat16)


def shard_levels(rng, dims, pieces, smallest, largest):
    level = 1.0
    for position, blocks in pieces:
        heights = jax.random.uniform(jax.random.fold_in(jax.random.fold_in(rng, 6), position), (blocks,), jnp.float32, smallest / len(pieces), largest / len(pieces))
        level = level * jnp.repeat(jnp.exp(heights), dims[position] // blocks).reshape((-1,) + (1,) * (len(dims) - 1 - position))
    return level


def scatter_about(stream_key, extent, width, bound, pieces=(), kind=jnp.bfloat16):
    array = width * jax.random.normal(stream_key, extent, jnp.float32)
    if pieces:
        array = array * shard_levels(stream_key, extent, pieces, -0.22, 0.18)
    return jnp.clip(array, -bound, bound).astype(kind)


def setup_inputs(seed: int = 0) -> dict:
    key_of = jax.random.split(jax.random.key(seed), 5)
    field = scatter_about(key_of[0], (B, C, NX, NY, NZ), 1.0, 6.0, ((2, 8), (3, 4)))
    spectral_weight = draw_spectral_weight(jax.random.fold_in(key_of[4], 71), 0)
    point_weight = scatter_about(key_of[2], (C, C), C ** -0.5, 1.0)
    point_bias = scatter_about(key_of[3], (C,), 0.5, 3.0, (), jnp.float32)
    return dict(field=field, spectral_weight=spectral_weight, point_weight=point_weight, point_bias=point_bias)


def contract(form, left, right):
    return jnp.einsum(form, left, right, precision=lax.Precision.HIGHEST, preferred_element_type=jnp.float32)


def reference(field, spectral_weight, point_weight, point_bias):
    batch = field.shape[0]
    channels = field.shape[1]
    index_x = jnp.concatenate([jnp.arange(MX // 2), jnp.arange(NX - MX // 2, NX)]).astype(jnp.int32)
    index_y = jnp.concatenate([jnp.arange(MY // 2), jnp.arange(NY - MY // 2, NY)]).astype(jnp.int32)
    index_z = jnp.arange(MZ).astype(jnp.int32)
    flat = field.reshape(batch * channels, NX, NY, NZ)

    def forward(single):
        full = jnp.fft.rfftn(single.astype(jnp.float32))
        kept = full[index_x][:, index_y][:, :, :MZ]
        return jnp.real(kept), jnp.imag(kept)

    real_all, imag_all = lax.map(forward, flat)
    real_all = jnp.transpose(real_all.reshape(batch, channels, MX, MY, MZ), (0, 1, 4, 2, 3))
    imag_all = jnp.transpose(imag_all.reshape(batch, channels, MX, MY, MZ), (0, 1, 4, 2, 3))
    in_real = lax.optimization_barrier(real_all.astype(jnp.bfloat16)).astype(jnp.float32)
    in_imag = lax.optimization_barrier(imag_all.astype(jnp.bfloat16)).astype(jnp.float32)
    weight_real = spectral_weight[0].astype(jnp.float32)
    weight_imag = spectral_weight[1].astype(jnp.float32)
    mixed_real = contract('bckij,cokij->bokij', in_real, weight_real) - contract('bckij,cokij->bokij', in_imag, weight_imag)
    mixed_imag = contract('bckij,cokij->bokij', in_real, weight_imag) + contract('bckij,cokij->bokij', in_imag, weight_real)
    mixed_real = mixed_real.reshape(batch * channels, MZ, MX, MY)
    mixed_imag = mixed_imag.reshape(batch * channels, MZ, MX, MY)
    weights_f = point_weight.astype(jnp.float32)
    bias_f = point_bias.astype(jnp.float32)

    def inverse(item):
        number, part_real, part_imag = item
        sample = number // channels
        output_channel = number % channels
        placed_real = jnp.zeros((NX, NY, NZ // 2 + 1), part_real.dtype)
        placed_imag = jnp.zeros((NX, NY, NZ // 2 + 1), part_real.dtype)
        spot = (index_x[:, None, None], index_y[None, :, None], index_z[None, None, :])
        placed_real = placed_real.at[spot].set(jnp.transpose(part_real, (1, 2, 0)))
        placed_imag = placed_imag.at[spot].set(jnp.transpose(part_imag, (1, 2, 0)))
        spectral = jnp.fft.irfftn(lax.complex(placed_real, placed_imag), s=(NX, NY, NZ))
        inputs = lax.dynamic_index_in_dim(field, sample, 0, keepdims=False)
        row = lax.dynamic_index_in_dim(weights_f, output_channel, 0, keepdims=False)
        bias_one = lax.dynamic_index_in_dim(bias_f, output_channel, 0, keepdims=False)
        pointwise = jnp.einsum('c,cxyz->xyz', row, inputs.astype(jnp.float32), precision=lax.Precision.HIGHEST) + bias_one
        return jax.nn.gelu(spectral + pointwise, approximate=False).astype(jnp.bfloat16)

    numbers = jnp.arange(batch * channels).astype(jnp.int32)
    result = lax.map(inverse, (numbers, mixed_real, mixed_imag))
    return result.reshape(batch, channels, NX, NY, NZ)
```

```python
from functools import partial
import math

import jax
import jax.numpy as jnp
import numpy as np
from jax import lax
from jax.experimental import pallas as pl
from jax.experimental.pallas import tpu as pltpu
from jax.sharding import PartitionSpec as P

MX = 64
MY = 64
MZ = 32


def contract(form, left, right):
    return jnp.einsum(
        form, left, right, precision=lax.Precision.HIGHEST, preferred_element_type=jnp.float32
    )


def angle_table(length, count, signed):
    position = jnp.arange(length, dtype=jnp.int32)
    number = jnp.arange(count, dtype=jnp.int32)
    if signed:
        number = jnp.where(number < count // 2, number, number - count)
    product = position[:, None] * number[None, :] % length
    return 2.0 * math.pi / length * product.astype(jnp.float32)


def forward_x(piece, keep_count, cos_x, sin_x):
    real_part = piece[0]
    imag_part = piece[1]
    out_real = contract("ix,bcxm->bcim", cos_x, real_part) + contract(
        "ix,bcxm->bcim", sin_x, imag_part
    )
    out_imag = contract("ix,bcxm->bcim", cos_x, imag_part) - contract(
        "ix,bcxm->bcim", sin_x, real_part
    )
    return jnp.stack([out_real, out_imag], axis=0)


def inverse_z(piece, table):
    return contract("pbcxky,pkz->bcxyz", piece, table)


def plain_body(field, spectral_weight, point_weight, point_bias):
    batch, channels, rows_x, rows_y, depth = field.shape
    grid_x = rows_x * lax.axis_size("px")
    grid_y = rows_y * lax.axis_size("py")
    theta_x = angle_table(grid_x, MX, True)
    theta_y = angle_table(grid_y, MY, True)
    wide = field.astype(jnp.float32)
    count = MZ
    theta_z = angle_table(depth, count, False)
    z_real = contract("bcxyz,zk->bcxky", wide, jnp.cos(theta_z))
    z_imag = contract("bcxyz,zk->bcxky", wide, -jnp.sin(theta_z))
    along_z = jnp.stack([z_real, z_imag], axis=0).reshape(
        2, batch, channels, rows_x, count * rows_y
    )
    step_x = partial(
        forward_x, keep_count=MZ * rows_y, cos_x=jnp.cos(theta_x).T, sin_x=jnp.sin(theta_x).T
    )
    along_x = step_x(lax.all_to_all(along_z, "px", split_axis=2, concat_axis=3, tiled=True))
    shape = along_x.shape
    along_x = along_x.reshape(shape[0], shape[1], shape[2], shape[3], MZ, rows_y)
    moved = lax.all_to_all(along_x, "py", split_axis=4, concat_axis=5, tiled=True)
    cos_y = jnp.cos(theta_y)
    sin_y = jnp.sin(theta_y)
    spec_real = contract("bciky,yj->bcikj", moved[0], cos_y) + contract(
        "bciky,yj->bcikj", moved[1], sin_y
    )
    spec_imag = contract("bciky,yj->bcikj", moved[1], cos_y) - contract(
        "bciky,yj->bcikj", moved[0], sin_y
    )
    spectrum = jnp.stack([spec_real, spec_imag], axis=0).astype(jnp.bfloat16)
    gathered = lax.all_gather(spectrum, "px", axis=2, tiled=True)
    in_real = gathered[0].astype(jnp.float32)
    in_imag = gathered[1].astype(jnp.float32)
    weight_real = spectral_weight[0].astype(jnp.float32)
    weight_imag = spectral_weight[1].astype(jnp.float32)
    mixed_real = contract("bcikj,cokij->boikj", in_real, weight_real) - contract(
        "bcikj,cokij->boikj", in_imag, weight_imag
    )
    mixed_imag = contract("bcikj,cokij->boikj", in_real, weight_imag) + contract(
        "bcikj,cokij->boikj", in_imag, weight_real
    )
    cos_yt = jnp.cos(theta_y).T
    sin_yt = jnp.sin(theta_y).T
    back_real = contract("boikj,jy->boiky", mixed_real, cos_yt) - contract(
        "boikj,jy->boiky", mixed_imag, sin_yt
    )
    back_imag = contract("boikj,jy->boiky", mixed_real, sin_yt) + contract(
        "boikj,jy->boiky", mixed_imag, cos_yt
    )
    returned = lax.all_to_all(
        jnp.stack([back_real, back_imag], axis=0), "py", split_axis=5, concat_axis=4, tiled=True
    )
    cos_xt = jnp.cos(theta_x)
    sin_xt = jnp.sin(theta_x)
    out_real = contract("xi,boiky->boxky", cos_xt, returned[0]) - contract(
        "xi,boiky->boxky", sin_xt, returned[1]
    )
    out_imag = contract("xi,boiky->boxky", sin_xt, returned[0]) + contract(
        "xi,boiky->boxky", cos_xt, returned[1]
    )
    planes = jnp.stack([out_real, out_imag], axis=0)
    theta_back = angle_table(depth, MZ, False).T
    factor = jnp.where(jnp.arange(MZ) == 0, 1.0, 2.0).astype(jnp.float32) / float(
        grid_x * grid_y * depth
    )
    table_back = jnp.stack(
        [factor[:, None] * jnp.cos(theta_back), -factor[:, None] * jnp.sin(theta_back)], axis=0
    )
    spectral = inverse_z(
        lax.all_to_all(planes, "px", split_axis=3, concat_axis=2, tiled=True), table=table_back
    )
    pointwise = jnp.einsum(
        "oc,bcxyz->boxyz", point_weight, field, preferred_element_type=jnp.float32
    )
    pointwise = pointwise + point_bias[None, :, None, None, None]
    return jax.nn.gelu(spectral + pointwise, approximate=False).astype(jnp.bfloat16)


BF = jnp.bfloat16
F32 = jnp.float32
VMEM = pltpu.VMEM
LANES = 128


def signed_numbers(count):
    number = np.arange(count)
    return np.where(number < count // 2, number, number - count)


def angles(length, positions, numbers):
    return 2.0 * np.pi * (np.multiply.outer(positions, numbers) % length) / length


def constant(table):
    return jnp.asarray(np.asarray(table, np.float32), BF)


def whole(shape):
    return pl.BlockSpec(shape, lambda i: (0,) * len(shape))


def greet(axis, me, n):
    barrier = pltpu.get_barrier_semaphore()
    for k in range(1, n):
        pl.semaphore_signal(
            barrier, inc=1, device_id={axis: lax.rem(me + k, n)},
            device_id_type=pl.DeviceIdType.MESH,
        )
    pl.semaphore_wait(barrier, n - 1)


def exchange_kernel(axis, n, x_ref, o_ref, send_sem, recv_sem, own_sem):
    me = lax.axis_index(axis)
    greet(axis, me, n)
    copies = []
    for k in range(1, n):
        peer = lax.rem(me + k, n)
        copy = pltpu.make_async_remote_copy(
            src_ref=x_ref.at[peer], dst_ref=o_ref.at[me],
            send_sem=send_sem.at[k], recv_sem=recv_sem.at[k],
            device_id={axis: peer}, device_id_type=pl.DeviceIdType.MESH,
        )
        copy.start()
        copies.append(copy)
    own = pltpu.make_async_copy(x_ref.at[me], o_ref.at[me], own_sem)
    own.start()
    own.wait()
    for copy in copies:
        copy.wait()


def exchange(x, axis, n, number):
    return pl.pallas_call(
        partial(exchange_kernel, axis, n),
        out_shape=jax.ShapeDtypeStruct(x.shape, x.dtype),
        in_specs=[pl.BlockSpec(memory_space=VMEM)],
        out_specs=pl.BlockSpec(memory_space=VMEM),
        scratch_shapes=[
            pltpu.SemaphoreType.DMA((n,)), pltpu.SemaphoreType.DMA((n,)), pltpu.SemaphoreType.DMA
        ],
        compiler_params=pltpu.CompilerParams(collective_id=number, has_side_effects=True),
        name=f"exchange_{axis}_{number}",
    )(x)


def gather_kernel(axis, n, x_ref, o_ref, up_send, up_recv, down_send, down_recv, side_send, side_recv, own_sem):
    me = lax.axis_index(axis)
    rows = n // 2
    h = me // 2
    s = me % 2
    greet(axis, me, n)

    def copy_to(source_row, first, send, recv, peer):
        place = source_row * 2 + s
        return pltpu.make_async_remote_copy(
            src_ref=x_ref if first else o_ref.at[place], dst_ref=o_ref.at[place],
            send_sem=send, recv_sem=recv,
            device_id={axis: peer}, device_id_type=pl.DeviceIdType.MESH,
        )

    def up(d):
        return copy_to(h - d, d == 0, up_send.at[d], up_recv.at[d], me + 2)

    def down(d):
        return copy_to(h + d, d == 0, down_send.at[d], down_recv.at[d], me - 2)

    def side(row, first):
        return copy_to(row, first, side_send.at[row], side_recv.at[row], h * 2 + 1 - s)

    def arrived(row, recv):
        place = row * 2 + s
        pltpu.make_async_remote_copy(
            src_ref=o_ref.at[place], dst_ref=o_ref.at[place], send_sem=own_sem, recv_sem=recv,
            device_id={axis: h * 2 + 1 - s}, device_id_type=pl.DeviceIdType.MESH,
        ).wait_recv()

    pl.when(h < rows - 1)(lambda: up(0).start())
    pl.when(h > 0)(lambda: down(0).start())
    side(h, True).start()
    own = pltpu.make_async_copy(x_ref, o_ref.at[me], own_sem)
    own.start()
    own.wait()
    for d in range(1, rows):

        @pl.when(h - d >= 0)
        def _():
            arrived(h - d, up_recv.at[d - 1])
            pl.when(h < rows - 1)(lambda: up(d).start())
            side(h - d, False).start()

        @pl.when(h + d <= rows - 1)
        def _():
            arrived(h + d, down_recv.at[d - 1])
            pl.when(h > 0)(lambda: down(d).start())
            side(h + d, False).start()

    for row in range(rows):
        pltpu.make_async_remote_copy(
            src_ref=o_ref.at[row * 2 + 1 - s], dst_ref=o_ref.at[row * 2 + 1 - s],
            send_sem=side_send.at[row], recv_sem=side_recv.at[row],
            device_id={axis: h * 2 + 1 - s}, device_id_type=pl.DeviceIdType.MESH,
        ).wait()
    for d in range(rows):
        pl.when((h - d >= 0) & (h < rows - 1))(lambda: up(d).wait_send())
        pl.when((h + d <= rows - 1) & (h > 0))(lambda: down(d).wait_send())


def gather(x, axis, n, number):
    rows = n // 2
    return pl.pallas_call(
        partial(gather_kernel, axis, n),
        out_shape=jax.ShapeDtypeStruct((n,) + x.shape, x.dtype),
        in_specs=[pl.BlockSpec(memory_space=VMEM)],
        out_specs=pl.BlockSpec(memory_space=VMEM),
        scratch_shapes=[pltpu.SemaphoreType.DMA((rows,))] * 6 + [pltpu.SemaphoreType.DMA],
        compiler_params=pltpu.CompilerParams(collective_id=number, has_side_effects=True),
        name="gather",
    )(x)


def forward_z_kernel(f_ref, t_ref, o_ref):
    parts, tiles, kept, lanes = o_ref.shape
    r = lax.dot_general(t_ref[...], f_ref[...], (((1,), (1,)), ((), ())), preferred_element_type=F32)
    r = r.astype(BF)
    for q in range(parts):
        for t in range(tiles):
            o_ref[q, t] = r[q * kept:(q + 1) * kept, t * lanes:(t + 1) * lanes]


def forward_y_kernel(a_ref, t_ref, o_ref):
    parts, tiles, kept, lanes = a_ref.shape
    left = jnp.concatenate([a_ref[q].reshape(tiles * kept, lanes) for q in range(parts)], axis=1)
    r = jnp.dot(left, t_ref[...], preferred_element_type=F32)
    half = r.shape[1] // 2
    r = r.reshape(tiles, 2, kept // 2, 2 * half)
    r = r[:, 0, :, :half] + r[:, 1, :, half:]
    o_ref[...] = r.reshape(o_ref.shape).astype(BF)


def forward_x_kernel(a_ref, t_ref, o_ref):
    depth = o_ref.shape[1]
    v = a_ref[...].astype(F32)
    blocks, rows, wide = v.shape
    v = v.reshape(blocks * rows // depth, depth, wide)
    pieces = [
        jnp.swapaxes(v[:, :, g * LANES:(g + 1) * LANES], 0, 1) for g in range(wide // LANES)
    ]
    stacked = jnp.concatenate(pieces, axis=1).astype(BF)
    lane = lax.broadcasted_iota(jnp.int32, (MX, LANES), 1)
    for l in range(depth):
        r = jnp.dot(t_ref[...], stacked[l], preferred_element_type=F32)
        turned = pltpu.roll(r[MX:], MY, 1)
        o_ref[0, l] = (r[:MX] + jnp.where(lane < MY, turned, -turned)).astype(BF)


def mix_kernel(s_ref, w_ref, t_ref, o_ref, held):
    channels, depth = s_ref.shape[:2]

    def one(l, carry):
        real = jnp.zeros((MX, MY), F32)
        imag = jnp.zeros((MX, MY), F32)
        for c in range(channels):
            s = s_ref[c, l].astype(F32)
            s_real, s_imag = s[:, :MY], s[:, MY:]
            w_real = w_ref[0, c, 0, l].astype(F32)
            w_imag = w_ref[1, c, 0, l].astype(F32)
            real = real + (s_real * w_real - s_imag * w_imag)
            imag = imag + (s_real * w_imag + s_imag * w_real)
        both = jnp.concatenate([real, imag], axis=1)
        turned = jnp.concatenate([-imag, real], axis=1)
        stacked = jnp.concatenate([both, turned], axis=0).astype(BF)
        held[l] = jnp.dot(t_ref[...], stacked, preferred_element_type=F32)
        return carry

    lax.fori_loop(0, depth, one, 0)
    blocks, rows, wide = o_ref.shape
    count = wide // LANES
    step = held.shape[1] // count
    for g in range(count):
        v = jnp.swapaxes(held[:, g * step:(g + 1) * step, :], 0, 1)
        o_ref[:, :, g * LANES:(g + 1) * LANES] = v.reshape(blocks, rows, LANES).astype(BF)


def inverse_y_kernel(a_ref, t_ref, o_ref):
    parts, tiles, kept, lanes = o_ref.shape
    r = jnp.dot(a_ref[0], t_ref[...], preferred_element_type=F32)
    r = r.reshape(tiles, kept // 2, r.shape[1])
    for q in range(parts):
        first = 2 * q * lanes
        o_ref[q] = jnp.concatenate(
            [r[:, :, first:first + lanes], r[:, :, first + lanes:first + 2 * lanes]], axis=1
        ).astype(BF)


def final_kernel(a_ref, f_ref, t_ref, k_ref, b_ref, o_ref, held):
    parts, channels = a_ref.shape[:2]
    rows = f_ref.shape[1]
    depth = f_ref.shape[2]

    def one(o, carry):
        left = jnp.concatenate([a_ref[q, o, 0] for q in range(parts)], axis=0)
        held[o] = lax.dot_general(
            left, t_ref[...], (((0,), (0,)), ((), ())), preferred_element_type=F32
        )
        return carry

    lax.fori_loop(0, channels, one, 0, unroll=4)
    sub = k_ref.shape[0] // channels

    def two(r, carry):
        spot = pl.ds(pl.multiple_of(r * sub, sub), sub)
        f = f_ref[:, spot, :].reshape(channels * sub, depth)
        v = jnp.dot(k_ref[...], f, preferred_element_type=F32) + b_ref[...]
        v = v + held[:, spot, :].reshape(channels * sub, depth)
        v = 0.5 * v * (1.0 + lax.erf(v * math.sqrt(0.5)))
        o_ref[:, spot, :] = v.reshape(channels, sub, depth).astype(BF)
        return carry

    lax.fori_loop(0, rows // sub, two, 0)


def body(field, spectral_weight, point_weight, point_bias):
    batch, channels, rows_x, rows_y, depth = field.shape
    n_p = lax.axis_size("px")
    n_q = lax.axis_size("py")
    group = max(1, LANES // rows_y)
    own_l = MZ // n_q
    own_c = channels // n_p
    if (
        batch != 1 or group * rows_y != LANES or rows_x % group or own_l % 8
        or channels % n_p or n_p % 2 or 2 * MY != LANES
    ):
        return plain_body(field, spectral_weight, point_weight, point_bias)
    grid_x, grid_y = rows_x * n_p, rows_y * n_q
    tiles_x = rows_x // group
    tiles = channels * tiles_x
    kept = 2 * own_l
    wide = group * LANES
    steps = n_p
    per_step = tiles // steps

    theta = angles(depth, np.arange(depth), np.arange(MZ))
    table_z = np.stack([np.cos(theta), -np.sin(theta)]).reshape(2, depth, n_q, own_l)
    table_z = table_z.transpose(2, 0, 3, 1).reshape(n_q * kept, depth)
    weight = np.where(np.arange(MZ) == 0, 1.0, 2.0) / float(grid_x * grid_y * depth)
    back_z = np.stack([np.cos(theta) * weight, -np.sin(theta) * weight])
    back_z = back_z.reshape(2, depth, n_q, own_l).transpose(2, 0, 3, 1).reshape(n_q * kept, depth)

    theta = angles(grid_y, np.arange(grid_y), signed_numbers(MY))
    cos_y, sin_y = np.cos(theta), np.sin(theta)
    eye = np.eye(group)
    rule = np.stack([np.stack([cos_y, -sin_y], 1), np.stack([sin_y, cos_y], 1)])
    rule = rule.reshape(2, n_q, rows_y, 2, MY)
    table_y = np.einsum("uqyrj,gh->qgyuhrj", rule, eye).reshape(n_q * LANES, 2 * wide)
    rule = np.stack([np.stack([cos_y, sin_y]), np.stack([-sin_y, cos_y])])
    rule = rule.reshape(2, 2, n_q, rows_y, MY)
    back_y = np.einsum("urqyj,gh->gujqrhy", rule, eye).reshape(wide, 2 * n_q * LANES)

    order = np.arange(grid_x).reshape(n_p * tiles_x, group).T.reshape(-1)
    theta = angles(grid_x, order, signed_numbers(MX))
    table_x = np.concatenate([np.cos(theta).T, np.sin(theta).T], axis=0)
    back_x = np.concatenate([np.cos(theta), np.sin(theta)], axis=1)

    along_z = pl.pallas_call(
        forward_z_kernel,
        grid=(steps,),
        in_specs=[
            pl.BlockSpec((per_step * LANES, depth), lambda i: (i, 0)),
            whole(table_z.shape),
        ],
        out_specs=pl.BlockSpec((n_q, per_step, kept, LANES), lambda i: (0, i, 0, 0)),
        out_shape=jax.ShapeDtypeStruct((n_q, tiles, kept, LANES), BF),
        name="forward_z",
    )(field.reshape(tiles * LANES, depth), constant(table_z))
    along_z = exchange(along_z, "py", n_q, 1)
    along_y = pl.pallas_call(
        forward_y_kernel,
        grid=(steps,),
        in_specs=[
            pl.BlockSpec((n_q, per_step, kept, LANES), lambda i: (0, i, 0, 0)),
            whole(table_y.shape),
        ],
        out_specs=pl.BlockSpec((1, per_step * own_l, wide), lambda i: (i, 0, 0)),
        out_shape=jax.ShapeDtypeStruct((n_p, per_step * own_l, wide), BF),
        name="forward_y",
    )(along_z, constant(table_y))
    along_y = exchange(along_y, "px", n_p, 2)
    spectrum = pl.pallas_call(
        forward_x_kernel,
        grid=(own_c,),
        in_specs=[
            pl.BlockSpec((n_p, tiles_x * own_l, wide), lambda i: (0, i, 0)),
            whole(table_x.shape),
        ],
        out_specs=pl.BlockSpec((1, own_l, MX, LANES), lambda i: (i, 0, 0, 0)),
        out_shape=jax.ShapeDtypeStruct((own_c, own_l, MX, LANES), BF),
        name="forward_x",
    )(along_y, constant(table_x))
    spectrum = gather(spectrum, "px", n_p, 3).reshape(channels, own_l, MX, LANES)
    mixed = pl.pallas_call(
        mix_kernel,
        grid=(own_c,),
        in_specs=[
            whole(spectrum.shape),
            pl.BlockSpec((2, channels, 1, own_l, MX, MY), lambda i: (0, 0, i, 0, 0, 0)),
            whole(back_x.shape),
        ],
        out_specs=pl.BlockSpec((n_p, tiles_x * own_l, wide), lambda i: (0, i, 0)),
        out_shape=jax.ShapeDtypeStruct((n_p, own_c * tiles_x * own_l, wide), BF),
        scratch_shapes=[pltpu.VMEM((own_l, grid_x, LANES), F32)],
        name="mix",
    )(spectrum, spectral_weight, constant(back_x))
    mixed = exchange(mixed, "px", n_p, 4)
    planes = pl.pallas_call(
        inverse_y_kernel,
        grid=(steps,),
        in_specs=[
            pl.BlockSpec((1, per_step * own_l, wide), lambda i: (i, 0, 0)),
            whole(back_y.shape),
        ],
        out_specs=pl.BlockSpec((n_q, per_step, kept, LANES), lambda i: (0, i, 0, 0)),
        out_shape=jax.ShapeDtypeStruct((n_q, tiles, kept, LANES), BF),
        name="inverse_y",
    )(mixed, constant(back_y))
    planes = exchange(planes, "py", n_q, 5)
    planes = planes.reshape(n_q, channels, tiles_x, kept, LANES)
    sub = 16
    spread = (
        point_weight[:, None, :, None] * jnp.eye(sub, dtype=BF)[None, :, None, :]
    ).reshape(channels * sub, channels * sub)
    bias = jnp.repeat(point_bias, sub)[:, None]
    out = pl.pallas_call(
        final_kernel,
        grid=(tiles_x,),
        in_specs=[
            pl.BlockSpec((n_q, channels, 1, kept, LANES), lambda i: (0, 0, i, 0, 0)),
            pl.BlockSpec((channels, LANES, depth), lambda i: (0, i, 0)),
            whole(back_z.shape),
            whole(spread.shape),
            whole(bias.shape),
        ],
        out_specs=pl.BlockSpec((channels, LANES, depth), lambda i: (0, i, 0)),
        out_shape=jax.ShapeDtypeStruct((channels, rows_x * rows_y, depth), BF),
        scratch_shapes=[pltpu.VMEM((channels, LANES, depth), F32)],
        name="final",
    )(planes, field.reshape(channels, rows_x * rows_y, depth), constant(back_z), spread, bias)
    return out.reshape(field.shape)


def solution(mesh):
    placed = (P(None, None, "px", "py", None), P(None, None, "px", "py", None, None), P(), P())
    return jax.shard_map(
        body, mesh=mesh, in_specs=placed, out_specs=P(None, None, "px", "py", None), check_vma=False
    )
```

```python
from functools import partial
import math

import jax
import jax.numpy as jnp
import numpy as np
from jax import lax
from jax.experimental import pallas as pl
from jax.experimental.pallas import tpu as pltpu
from jax.sharding import PartitionSpec as P

MX = 64
MY = 64
MZ = 32


def contract(form, left, right):
    return jnp.einsum(
        form, left, right, precision=lax.Precision.HIGHEST, preferred_element_type=jnp.float32
    )


def angle_table(length, count, signed):
    position = jnp.arange(length, dtype=jnp.int32)
    number = jnp.arange(count, dtype=jnp.int32)
    if signed:
        number = jnp.where(number < count // 2, number, number - count)
    product = position[:, None] * number[None, :] % length
    return 2.0 * math.pi / length * product.astype(jnp.float32)


def forward_x(piece, keep_count, cos_x, sin_x):
    real_part = piece[0]
    imag_part = piece[1]
    out_real = contract("ix,bcxm->bcim", cos_x, real_part) + contract(
        "ix,bcxm->bcim", sin_x, imag_part
    )
    out_imag = contract("ix,bcxm->bcim", cos_x, imag_part) - contract(
        "ix,bcxm->bcim", sin_x, real_part
    )
    return jnp.stack([out_real, out_imag], axis=0)


def inverse_z(piece, table):
    return contract("pbcxky,pkz->bcxyz", piece, table)


def plain_body(field, spectral_weight, point_weight, point_bias):
    batch, channels, rows_x, rows_y, depth = field.shape
    grid_x = rows_x * lax.axis_size("px")
    grid_y = rows_y * lax.axis_size("py")
    theta_x = angle_table(grid_x, MX, True)
    theta_y = angle_table(grid_y, MY, True)
    wide = field.astype(jnp.float32)
    count = MZ
    theta_z = angle_table(depth, count, False)
    z_real = contract("bcxyz,zk->bcxky", wide, jnp.cos(theta_z))
    z_imag = contract("bcxyz,zk->bcxky", wide, -jnp.sin(theta_z))
    along_z = jnp.stack([z_real, z_imag], axis=0).reshape(
        2, batch, channels, rows_x, count * rows_y
    )
    step_x = partial(
        forward_x, keep_count=MZ * rows_y, cos_x=jnp.cos(theta_x).T, sin_x=jnp.sin(theta_x).T
    )
    along_x = step_x(lax.all_to_all(along_z, "px", split_axis=2, concat_axis=3, tiled=True))
    shape = along_x.shape
    along_x = along_x.reshape(shape[0], shape[1], shape[2], shape[3], MZ, rows_y)
    moved = lax.all_to_all(along_x, "py", split_axis=4, concat_axis=5, tiled=True)
    cos_y = jnp.cos(theta_y)
    sin_y = jnp.sin(theta_y)
    spec_real = contract("bciky,yj->bcikj", moved[0], cos_y) + contract(
        "bciky,yj->bcikj", moved[1], sin_y
    )
    spec_imag = contract("bciky,yj->bcikj", moved[1], cos_y) - contract(
        "bciky,yj->bcikj", moved[0], sin_y
    )
    spectrum = jnp.stack([spec_real, spec_imag], axis=0).astype(jnp.bfloat16)
    gathered = lax.all_gather(spectrum, "px", axis=2, tiled=True)
    in_real = gathered[0].astype(jnp.float32)
    in_imag = gathered[1].astype(jnp.float32)
    weight_real = spectral_weight[0].astype(jnp.float32)
    weight_imag = spectral_weight[1].astype(jnp.float32)
    mixed_real = contract("bcikj,cokij->boikj", in_real, weight_real) - contract(
        "bcikj,cokij->boikj", in_imag, weight_imag
    )
    mixed_imag = contract("bcikj,cokij->boikj", in_real, weight_imag) + contract(
        "bcikj,cokij->boikj", in_imag, weight_real
    )
    cos_yt = jnp.cos(theta_y).T
    sin_yt = jnp.sin(theta_y).T
    back_real = contract("boikj,jy->boiky", mixed_real, cos_yt) - contract(
        "boikj,jy->boiky", mixed_imag, sin_yt
    )
    back_imag = contract("boikj,jy->boiky", mixed_real, sin_yt) + contract(
        "boikj,jy->boiky", mixed_imag, cos_yt
    )
    returned = lax.all_to_all(
        jnp.stack([back_real, back_imag], axis=0), "py", split_axis=5, concat_axis=4, tiled=True
    )
    cos_xt = jnp.cos(theta_x)
    sin_xt = jnp.sin(theta_x)
    out_real = contract("xi,boiky->boxky", cos_xt, returned[0]) - contract(
        "xi,boiky->boxky", sin_xt, returned[1]
    )
    out_imag = contract("xi,boiky->boxky", sin_xt, returned[0]) + contract(
        "xi,boiky->boxky", cos_xt, returned[1]
    )
    planes = jnp.stack([out_real, out_imag], axis=0)
    theta_back = angle_table(depth, MZ, False).T
    factor = jnp.where(jnp.arange(MZ) == 0, 1.0, 2.0).astype(jnp.float32) / float(
        grid_x * grid_y * depth
    )
    table_back = jnp.stack(
        [factor[:, None] * jnp.cos(theta_back), -factor[:, None] * jnp.sin(theta_back)], axis=0
    )
    spectral = inverse_z(
        lax.all_to_all(planes, "px", split_axis=3, concat_axis=2, tiled=True), table=table_back
    )
    pointwise = jnp.einsum(
        "oc,bcxyz->boxyz", point_weight, field, preferred_element_type=jnp.float32
    )
    pointwise = pointwise + point_bias[None, :, None, None, None]
    return jax.nn.gelu(spectral + pointwise, approximate=False).astype(jnp.bfloat16)


BF = jnp.bfloat16
F32 = jnp.float32
VMEM = pltpu.VMEM
LANES = 128


def signed_numbers(count):
    number = np.arange(count)
    return np.where(number < count // 2, number, number - count)


def angles(length, positions, numbers):
    return 2.0 * np.pi * (np.multiply.outer(positions, numbers) % length) / length


def constant(table):
    return jnp.asarray(np.asarray(table, np.float32), BF)


def whole(shape):
    return pl.BlockSpec(shape, lambda i: (0,) * len(shape))


def greet(axis, me, n):
    barrier = pltpu.get_barrier_semaphore()
    for k in range(1, n):
        pl.semaphore_signal(
            barrier, inc=1, device_id={axis: lax.rem(me + k, n)},
            device_id_type=pl.DeviceIdType.MESH,
        )
    pl.semaphore_wait(barrier, n - 1)


def exchange_kernel(axis, n, x_ref, o_ref, send_sem, recv_sem, own_sem):
    me = lax.axis_index(axis)
    greet(axis, me, n)
    copies = []
    for k in range(1, n):
        peer = lax.rem(me + k, n)
        copy = pltpu.make_async_remote_copy(
            src_ref=x_ref.at[peer], dst_ref=o_ref.at[me],
            send_sem=send_sem.at[k], recv_sem=recv_sem.at[k],
            device_id={axis: peer}, device_id_type=pl.DeviceIdType.MESH,
        )
        copy.start()
        copies.append(copy)
    own = pltpu.make_async_copy(x_ref.at[me], o_ref.at[me], own_sem)
    own.start()
    own.wait()
    for copy in copies:
        copy.wait()


def exchange(x, axis, n, number):
    return pl.pallas_call(
        partial(exchange_kernel, axis, n),
        out_shape=jax.ShapeDtypeStruct(x.shape, x.dtype),
        in_specs=[pl.BlockSpec(memory_space=VMEM)],
        out_specs=pl.BlockSpec(memory_space=VMEM),
        scratch_shapes=[
            pltpu.SemaphoreType.DMA((n,)), pltpu.SemaphoreType.DMA((n,)), pltpu.SemaphoreType.DMA
        ],
        compiler_params=pltpu.CompilerParams(collective_id=number, has_side_effects=True),
        name=f"exchange_{axis}_{number}",
    )(x)


def gather_kernel(axis, n, x_ref, o_ref, up_send, up_recv, down_send, down_recv, side_send, side_recv, own_sem):
    me = lax.axis_index(axis)
    rows = n // 2
    h = me // 2
    s = me % 2
    greet(axis, me, n)

    def copy_to(source_row, first, send, recv, peer):
        place = source_row * 2 + s
        return pltpu.make_async_remote_copy(
            src_ref=x_ref if first else o_ref.at[place], dst_ref=o_ref.at[place],
            send_sem=send, recv_sem=recv,
            device_id={axis: peer}, device_id_type=pl.DeviceIdType.MESH,
        )

    def up(d):
        return copy_to(h - d, d == 0, up_send.at[d], up_recv.at[d], me + 2)

    def down(d):
        return copy_to(h + d, d == 0, down_send.at[d], down_recv.at[d], me - 2)

    def side(row, first):
        return copy_to(row, first, side_send.at[row], side_recv.at[row], h * 2 + 1 - s)

    def arrived(row, recv):
        place = row * 2 + s
        pltpu.make_async_remote_copy(
            src_ref=o_ref.at[place], dst_ref=o_ref.at[place], send_sem=own_sem, recv_sem=recv,
            device_id={axis: h * 2 + 1 - s}, device_id_type=pl.DeviceIdType.MESH,
        ).wait_recv()

    pl.when(h < rows - 1)(lambda: up(0).start())
    pl.when(h > 0)(lambda: down(0).start())
    side(h, True).start()
    own = pltpu.make_async_copy(x_ref, o_ref.at[me], own_sem)
    own.start()
    own.wait()
    for d in range(1, rows):

        @pl.when(h - d >= 0)
        def _():
            arrived(h - d, up_recv.at[d - 1])
            pl.when(h < rows - 1)(lambda: up(d).start())
            side(h - d, False).start()

        @pl.when(h + d <= rows - 1)
        def _():
            arrived(h + d, down_recv.at[d - 1])
            pl.when(h > 0)(lambda: down(d).start())
            side(h + d, False).start()

    for row in range(rows):
        pltpu.make_async_remote_copy(
            src_ref=o_ref.at[row * 2 + 1 - s], dst_ref=o_ref.at[row * 2 + 1 - s],
            send_sem=side_send.at[row], recv_sem=side_recv.at[row],
            device_id={axis: h * 2 + 1 - s}, device_id_type=pl.DeviceIdType.MESH,
        ).wait()
    for d in range(rows):
        pl.when((h - d >= 0) & (h < rows - 1))(lambda: up(d).wait_send())
        pl.when((h + d <= rows - 1) & (h > 0))(lambda: down(d).wait_send())


def gather(x, axis, n, number):
    rows = n // 2
    return pl.pallas_call(
        partial(gather_kernel, axis, n),
        out_shape=jax.ShapeDtypeStruct((n,) + x.shape, x.dtype),
        in_specs=[pl.BlockSpec(memory_space=VMEM)],
        out_specs=pl.BlockSpec(memory_space=VMEM),
        scratch_shapes=[pltpu.SemaphoreType.DMA((rows,))] * 6 + [pltpu.SemaphoreType.DMA],
        compiler_params=pltpu.CompilerParams(collective_id=number, has_side_effects=True),
        name="gather",
    )(x)


def forward_z_kernel(f_ref, t_ref, o_ref):
    parts, tiles, kept, lanes = o_ref.shape
    r = lax.dot_general(t_ref[...], f_ref[...], (((1,), (1,)), ((), ())), preferred_element_type=F32)
    r = r.astype(BF)
    for q in range(parts):
        for t in range(tiles):
            o_ref[q, t] = r[q * kept:(q + 1) * kept, t * lanes:(t + 1) * lanes]


def forward_y_kernel(a_ref, t_ref, o_ref):
    parts, tiles, kept, lanes = a_ref.shape
    left = jnp.concatenate([a_ref[q].reshape(tiles * kept, lanes) for q in range(parts)], axis=1)
    r = jnp.dot(left, t_ref[...], preferred_element_type=F32)
    half = r.shape[1] // 2
    r = r.reshape(tiles, 2, kept // 2, 2 * half)
    r = r[:, 0, :, :half] + r[:, 1, :, half:]
    o_ref[...] = r.reshape(o_ref.shape).astype(BF)


def forward_x_kernel(a_ref, t_ref, o_ref):
    depth = o_ref.shape[1]
    v = a_ref[...].astype(F32)
    blocks, rows, wide = v.shape
    v = v.reshape(blocks * rows // depth, depth, wide)
    pieces = [
        jnp.swapaxes(v[:, :, g * LANES:(g + 1) * LANES], 0, 1) for g in range(wide // LANES)
    ]
    stacked = jnp.concatenate(pieces, axis=1).astype(BF)
    lane = lax.broadcasted_iota(jnp.int32, (MX, LANES), 1)
    for l in range(depth):
        r = jnp.dot(t_ref[...], stacked[l], preferred_element_type=F32)
        turned = pltpu.roll(r[MX:], MY, 1)
        o_ref[0, l] = (r[:MX] + jnp.where(lane < MY, turned, -turned)).astype(BF)


def mix_kernel(s_ref, w_ref, t_ref, o_ref, held, twin, total):
    channels, depth = s_ref.shape[:2]
    strip = 32

    @pl.when(pl.program_id(0) == 0)
    def _():
        def double(c, carry):
            for l in range(depth):
                s = s_ref[c, l]
                twin[0, c, l] = jnp.concatenate([s[:, :MY], s[:, :MY]], axis=1)
                twin[1, c, l] = jnp.concatenate([s[:, MY:], s[:, MY:]], axis=1)
            return carry

        lax.fori_loop(0, channels, double, 0)

    def one(l, carry):
        def piece(k, inner):
            spot = pl.ds(pl.multiple_of(k * strip, strip), strip)
            first = jnp.zeros((strip, LANES), F32)
            second = jnp.zeros((strip, LANES), F32)
            for c in range(channels):
                w = jnp.concatenate(
                    [w_ref[0, c, 0, l, spot, :], w_ref[1, c, 0, l, spot, :]], axis=1
                ).astype(F32)
                first = first + twin[0, c, l, spot, :].astype(F32) * w
                second = second + twin[1, c, l, spot, :].astype(F32) * w
            total[0, spot, :] = first
            total[1, spot, :] = second
            return inner

        lax.fori_loop(0, MX // strip, piece, 0)
        lane = lax.broadcasted_iota(jnp.int32, (MX, LANES), 1)
        second = pltpu.roll(total[1], MY, 1)
        both = total[0] + jnp.where(lane < MY, -second, second)
        turned = pltpu.roll(both, MY, 1)
        turned = jnp.where(lane < MY, -turned, turned)
        stacked = jnp.concatenate([both, turned], axis=0).astype(BF)
        held[l] = jnp.dot(t_ref[...], stacked, preferred_element_type=F32)
        return carry

    lax.fori_loop(0, depth, one, 0)
    blocks, rows, wide = o_ref.shape
    count = wide // LANES
    step = held.shape[1] // count
    for g in range(count):
        v = jnp.swapaxes(held[:, g * step:(g + 1) * step, :], 0, 1)
        o_ref[:, :, g * LANES:(g + 1) * LANES] = v.reshape(blocks, rows, LANES).astype(BF)


def inverse_y_kernel(a_ref, t_ref, o_ref):
    parts, tiles, kept, lanes = o_ref.shape
    r = jnp.dot(a_ref[0], t_ref[...], preferred_element_type=F32)
    r = r.reshape(tiles, kept // 2, r.shape[1])
    for q in range(parts):
        first = 2 * q * lanes
        o_ref[q] = jnp.concatenate(
            [r[:, :, first:first + lanes], r[:, :, first + lanes:first + 2 * lanes]], axis=1
        ).astype(BF)


def final_kernel(a_ref, f_ref, t_ref, e_ref, p_ref, b_ref, o_ref, held, k_ref):
    parts, channels = a_ref.shape[:2]
    rows = f_ref.shape[1]
    depth = f_ref.shape[2]
    sub = k_ref.shape[0] // channels

    @pl.when(pl.program_id(0) == 0)
    def _():
        tall = jnp.dot(e_ref[...], p_ref[...], preferred_element_type=F32).astype(BF)
        full = lax.dot_general(
            tall, e_ref[...], (((1,), (1,)), ((), ())), preferred_element_type=F32
        )
        row = lax.broadcasted_iota(jnp.int32, full.shape, 0)
        column = lax.broadcasted_iota(jnp.int32, full.shape, 1)
        k_ref[...] = jnp.where(row % sub == column % sub, full, 0.0).astype(BF)

    def one(o, carry):
        left = jnp.concatenate([a_ref[q, o, 0] for q in range(parts)], axis=0)
        held[o] = lax.dot_general(
            left, t_ref[...], (((0,), (0,)), ((), ())), preferred_element_type=F32
        ) + b_ref[o]
        return carry

    lax.fori_loop(0, channels, one, 0, unroll=4)

    def two(r, carry):
        spot = pl.ds(pl.multiple_of(r * sub, sub), sub)
        f = f_ref[:, spot, :].reshape(channels * sub, depth)
        v = jnp.dot(k_ref[...], f, preferred_element_type=F32)
        v = v + held[:, spot, :].reshape(channels * sub, depth)
        v = 0.5 * v * (1.0 + lax.erf(v * math.sqrt(0.5)))
        o_ref[:, spot, :] = v.reshape(channels, sub, depth).astype(BF)
        return carry

    lax.fori_loop(0, rows // sub, two, 0)


def body(field, spectral_weight, point_weight, point_bias):
    batch, channels, rows_x, rows_y, depth = field.shape
    n_p = lax.axis_size("px")
    n_q = lax.axis_size("py")
    group = max(1, LANES // rows_y)
    own_l = MZ // n_q
    own_c = channels // n_p
    if (
        batch != 1 or group * rows_y != LANES or rows_x % group or own_l % 8
        or channels % n_p or n_p % 2 or 2 * MY != LANES
    ):
        return plain_body(field, spectral_weight, point_weight, point_bias)
    grid_x, grid_y = rows_x * n_p, rows_y * n_q
    tiles_x = rows_x // group
    tiles = channels * tiles_x
    kept = 2 * own_l
    wide = group * LANES
    steps = n_p
    per_step = tiles // steps

    theta = angles(depth, np.arange(depth), np.arange(MZ))
    table_z = np.stack([np.cos(theta), -np.sin(theta)]).reshape(2, depth, n_q, own_l)
    table_z = table_z.transpose(2, 0, 3, 1).reshape(n_q * kept, depth)
    weight = np.where(np.arange(MZ) == 0, 1.0, 2.0) / float(grid_x * grid_y * depth)
    back_z = np.stack([np.cos(theta) * weight, -np.sin(theta) * weight])
    back_z = back_z.reshape(2, depth, n_q, own_l).transpose(2, 0, 3, 1).reshape(n_q * kept, depth)

    theta = angles(grid_y, np.arange(grid_y), signed_numbers(MY))
    cos_y, sin_y = np.cos(theta), np.sin(theta)
    eye = np.eye(group)
    rule = np.stack([np.stack([cos_y, -sin_y], 1), np.stack([sin_y, cos_y], 1)])
    rule = rule.reshape(2, n_q, rows_y, 2, MY)
    table_y = np.einsum("uqyrj,gh->qgyuhrj", rule, eye).reshape(n_q * LANES, 2 * wide)
    rule = np.stack([np.stack([cos_y, sin_y]), np.stack([-sin_y, cos_y])])
    rule = rule.reshape(2, 2, n_q, rows_y, MY)
    back_y = np.einsum("urqyj,gh->gujqrhy", rule, eye).reshape(wide, 2 * n_q * LANES)

    order = np.arange(grid_x).reshape(n_p * tiles_x, group).T.reshape(-1)
    theta = angles(grid_x, order, signed_numbers(MX))
    table_x = np.concatenate([np.cos(theta).T, np.sin(theta).T], axis=0)
    back_x = np.concatenate([np.cos(theta), np.sin(theta)], axis=1)

    along_z = pl.pallas_call(
        forward_z_kernel,
        grid=(steps,),
        in_specs=[
            pl.BlockSpec((per_step * LANES, depth), lambda i: (i, 0)),
            whole(table_z.shape),
        ],
        out_specs=pl.BlockSpec((n_q, per_step, kept, LANES), lambda i: (0, i, 0, 0)),
        out_shape=jax.ShapeDtypeStruct((n_q, tiles, kept, LANES), BF),
        name="forward_z",
    )(field.reshape(tiles * LANES, depth), constant(table_z))
    along_z = exchange(along_z, "py", n_q, 1)
    along_y = pl.pallas_call(
        forward_y_kernel,
        grid=(steps,),
        in_specs=[
            pl.BlockSpec((n_q, per_step, kept, LANES), lambda i: (0, i, 0, 0)),
            whole(table_y.shape),
        ],
        out_specs=pl.BlockSpec((1, per_step * own_l, wide), lambda i: (i, 0, 0)),
        out_shape=jax.ShapeDtypeStruct((n_p, per_step * own_l, wide), BF),
        name="forward_y",
    )(along_z, constant(table_y))
    along_y = exchange(along_y, "px", n_p, 2)
    spectrum = pl.pallas_call(
        forward_x_kernel,
        grid=(own_c,),
        in_specs=[
            pl.BlockSpec((n_p, tiles_x * own_l, wide), lambda i: (0, i, 0)),
            whole(table_x.shape),
        ],
        out_specs=pl.BlockSpec((1, own_l, MX, LANES), lambda i: (i, 0, 0, 0)),
        out_shape=jax.ShapeDtypeStruct((own_c, own_l, MX, LANES), BF),
        name="forward_x",
    )(along_y, constant(table_x))
    spectrum = gather(spectrum, "px", n_p, 3).reshape(channels, own_l, MX, LANES)
    mixed = pl.pallas_call(
        mix_kernel,
        grid=(own_c,),
        in_specs=[
            whole(spectrum.shape),
            pl.BlockSpec((2, channels, 1, own_l, MX, MY), lambda i: (0, 0, i, 0, 0, 0)),
            whole(back_x.shape),
        ],
        out_specs=pl.BlockSpec((n_p, tiles_x * own_l, wide), lambda i: (0, i, 0)),
        out_shape=jax.ShapeDtypeStruct((n_p, own_c * tiles_x * own_l, wide), BF),
        scratch_shapes=[
            pltpu.VMEM((own_l, grid_x, LANES), F32),
            pltpu.VMEM((2,) + spectrum.shape, BF),
            pltpu.VMEM((2, MX, LANES), F32),
        ],
        name="mix",
    )(spectrum, spectral_weight, constant(back_x))
    mixed = exchange(mixed, "px", n_p, 4)
    planes = pl.pallas_call(
        inverse_y_kernel,
        grid=(steps,),
        in_specs=[
            pl.BlockSpec((1, per_step * own_l, wide), lambda i: (i, 0, 0)),
            whole(back_y.shape),
        ],
        out_specs=pl.BlockSpec((n_q, per_step, kept, LANES), lambda i: (0, i, 0, 0)),
        out_shape=jax.ShapeDtypeStruct((n_q, tiles, kept, LANES), BF),
        name="inverse_y",
    )(mixed, constant(back_y))
    planes = exchange(planes, "py", n_q, 5)
    planes = planes.reshape(n_q, channels, tiles_x, kept, LANES)
    sub = 16
    spread = np.repeat(np.eye(channels), sub, axis=0)
    out = pl.pallas_call(
        final_kernel,
        grid=(tiles_x,),
        in_specs=[
            pl.BlockSpec((n_q, channels, 1, kept, LANES), lambda i: (0, 0, i, 0, 0)),
            pl.BlockSpec((channels, LANES, depth), lambda i: (0, i, 0)),
            whole(back_z.shape),
            whole(spread.shape),
            whole(point_weight.shape),
            pl.BlockSpec(memory_space=pltpu.SMEM),
        ],
        out_specs=pl.BlockSpec((channels, LANES, depth), lambda i: (0, i, 0)),
        out_shape=jax.ShapeDtypeStruct((channels, rows_x * rows_y, depth), BF),
        scratch_shapes=[
            pltpu.VMEM((channels, LANES, depth), F32),
            pltpu.VMEM((channels * sub, channels * sub), BF),
        ],
        name="final",
    )(
        planes, field.reshape(channels, rows_x * rows_y, depth), constant(back_z),
        constant(spread), point_weight, point_bias,
    )
    return out.reshape(field.shape)


def solution(mesh):
    placed = (P(None, None, "px", "py", None), P(None, None, "px", "py", None, None), P(), P())
    return jax.shard_map(
        body, mesh=mesh, in_specs=placed, out_specs=P(None, None, "px", "py", None), check_vma=False
    )
```
